32 devices in a mesh: py: 2 (over y), px: 4 (over x, core), pz: 4 (over z).
Axes of the slice: x: 2, y: 2, z: 4, core: 2. Of those that a mesh axis runs over, the one named last changes fastest.
Arguments:
- tracer: float32 [32, 512, 32, 128], P('py', 'px', 'pz'), may hold values from 0.2 to 1.8
- conductance: float32 [32, 512, 32, 128], P('py', 'px', 'pz'), may hold values from 0.03 to 0.15
- source: float32 [32, 512, 32, 128], P('py', 'px', 'pz'), may hold values from -0.2 to 0.2
Outputs:
- potential: float32 [32, 512, 32, 128], P('py', 'px', 'pz')
- tracer_end: float32 [32, 512, 32, 128], P('py', 'px', 'pz')
The draws below stay inside these ranges and needn't reach their ends.
All inputs are finite; a program needn't handle non-finite values.
Results may differ from the reference program's by a relative error of at most 0.00002.
Values sent between devices are 32-bit elements; how exact they have to be, the bound alone decides.
A program may use at most 320 MiB of HBM per device.

```python
import jax
import jax.numpy as jnp
from jax import lax

GRID_Y = 32
GRID_X = 512
GRID_Z = 32
MEMBERS = 128
STEPS = 4


def block_scale(stream_key, shape, shards, least, high):
    factor_of = 1.0
    for position, parts in shards:
        draws = jax.random.uniform(jax.random.fold_in(jax.random.fold_in(stream_key, 6), position), (parts,), jnp.float32, least / len(shards), high / len(shards))
        factor_of = factor_of * jnp.repeat(jnp.exp(draws), shape[position] // parts).reshape((-1,) + (1,) * (len(shape) - 1 - position))
    return factor_of


def setup_inputs(seed: int = 0) -> dict:
    splits = jax.random.split(jax.random.key(seed), 4)
    tracer = jnp.clip(0.2 + 1.5999999 * jax.random.uniform(splits[0], (GRID_Y, GRID_X, GRID_Z, MEMBERS), jnp.float32) ** block_scale(splits[0], (GRID_Y, GRID_X, GRID_Z, MEMBERS), ((0, 2), (1, 4), (2, 4)), -0.2, 0.2), 0.2, 1.8)
    conductance = jnp.clip(0.03 + 0.120000007 * jax.random.uniform(splits[1], (GRID_Y, GRID_X, GRID_Z, MEMBERS), jnp.float32) ** block_scale(splits[1], (GRID_Y, GRID_X, GRID_Z, MEMBERS), ((0, 2), (1, 4), (2, 4)), -0.2, 0.2), 0.03, 0.15)
    source = jnp.clip(jax.random.uniform(splits[2], (GRID_Y, GRID_X, GRID_Z, MEMBERS), jnp.float32, -0.2, 0.2) * block_scale(splits[2], (GRID_Y, GRID_X, GRID_Z, MEMBERS), ((0, 2), (1, 4), (2, 4)), -0.4, 0.0), -0.2, 0.2)
    return dict(tracer=tracer, conductance=conductance, source=source)


def strip_edges(values, dims):
    for dim in dims:
        values = lax.slice_in_dim(values, 1, values.shape[dim] - 1, axis=dim)
    return values


def neighbour(values, dim, start, dims):
    others = [other for other in dims if other != dim]
    values = strip_edges(values, others)
    return lax.slice_in_dim(values, start, start + values.shape[dim] - 2, axis=dim)


def one_step(padded, conductance, source):
    middle = strip_edges(padded, (0, 1, 2))
    lower = [neighbour(padded, dim, 0, (0, 1, 2)) for dim in (0, 1, 2)]
    upper = [neighbour(padded, dim, 2, (0, 1, 2)) for dim in (0, 1, 2)]
    spread = lower[0] + upper[0] + lower[1] + upper[1] + lower[2] + upper[2] - 6.0 * middle
    return middle + conductance * spread + source


def reference(tracer, conductance, source):
    for step in range(STEPS):
        tracer = one_step(jnp.pad(tracer, ((1, 1), (1, 1), (1, 1), (0, 0)), mode="wrap"), conductance, source)
    potential = jnp.cumsum(tracer, axis=2) / GRID_Z
    return potential, tracer
```

```python
import functools

import jax
import jax.numpy as jnp
from jax import lax
from jax.experimental import pallas as pl
from jax.experimental.pallas import tpu as pltpu
from jax.sharding import PartitionSpec as P

STEPS = 4
LAST = STEPS - 1
AXES = ("py", "px", "pz")
MESH = pl.DeviceIdType.MESH


def chunks_of(cells):
    for parts in (16, 8, 4, 2):
        if cells % (8 * parts) == 0:
            return parts
    raise ValueError("x extent")


def evolve(
    counts, parts, tracer, conductance, source, end, running,
    field, coeff, gain, zhalo, entering,
    load_sem, zsend, zrecv, ysend, yrecv, xsend, xrecv, psend, precv,
):
    rows_y, cells, deep, members = tracer.shape
    wide = cells // parts
    behind = parts // 2
    scale = 1.0 / (deep * counts[2])
    count = dict(zip(AXES, counts))
    mine = {axis: lax.axis_index(axis) for axis in count}
    after = {axis: lax.rem(mine[axis] + 1, count[axis]) for axis in count}
    before = {axis: lax.rem(mine[axis] + count[axis] - 1, count[axis]) for axis in count}
    lowest = mine["pz"] == 0
    highest = mine["pz"] == count["pz"] - 1
    body_y = pl.ds(1, rows_y)

    def span(c):
        return pl.ds(pl.multiple_of(c * wide, 8), wide)

    def inner(c, shift=0):
        return pl.ds(c * wide + 1 + shift, wide)

    def load(which, c):
        hbm, dst = (
            (tracer, field.at[0, body_y, inner(c)]),
            (conductance, coeff.at[:, span(c)]),
            (source, gain.at[:, span(c)]),
        )[which]
        return pltpu.make_async_copy(hbm.at[:, span(c)], dst, load_sem.at[which, c])

    def remote(src, dst, send, recv, axis, target):
        return pltpu.make_async_remote_copy(
            src_ref=src, dst_ref=dst, send_sem=send, recv_sem=recv,
            device_id={axis: target}, device_id_type=MESH,
        )

    def z_copy(t, side, c):
        p = lax.rem(t, 2)
        return remote(
            field.at[p, body_y, inner(c), (deep - 1, 0)[side]],
            zhalo.at[p, side, :, span(c)],
            zsend.at[p, side, c], zrecv.at[p, side, c],
            "pz", (after, before)[side]["pz"],
        )

    def y_copy(t, side, c):
        p = lax.rem(t, 2)
        return remote(
            field.at[p, (rows_y, 1)[side], inner(c)],
            field.at[p, (0, rows_y + 1)[side], inner(c)],
            ysend.at[p, side, c], yrecv.at[p, side, c],
            "py", (after, before)[side]["py"],
        )

    def x_copy(t, side):
        p = lax.rem(t, 2)
        return remote(
            field.at[p, body_y, (cells, 1)[side]],
            field.at[p, body_y, (0, cells + 1)[side]],
            xsend.at[p, side], xrecv.at[p, side],
            "px", (after, before)[side]["px"],
        )

    def prefix_copy(c):
        return remote(
            running.at[:, span(c), deep - 1], entering.at[:, span(c)],
            psend.at[c], precv.at[c], "pz", after["pz"],
        )

    def x_faces(t, c, act):
        @pl.when(c == 0)
        def _():
            act(x_copy(t, 1))

        @pl.when(c == parts - 1)
        def _():
            act(x_copy(t, 0))

    def send_faces(t, c):
        z_copy(t, 0, c).start()

        @pl.when(jnp.logical_or(t < LAST, mine["pz"] > 0))
        def _():
            z_copy(t, 1, c).start()

        for side in (0, 1):
            y_copy(t, side, c).start()
        x_faces(t, c, lambda copy: copy.start())

    def wait_sent(t, c):
        for side in (0, 1):
            z_copy(t, side, c).wait_send()
            y_copy(t, side, c).wait_send()
        x_faces(t, c, lambda copy: copy.wait_send())

    def wait_faces(t, c):
        for side in (0, 1):
            z_copy(t, side, c).wait_recv()
            y_copy(t, side, c).wait_recv()

        @pl.when(c == 0)
        def _():
            x_copy(t, 0).wait_recv()

        @pl.when(c == parts - 1)
        def _():
            x_copy(t, 1).wait_recv()

    def each(limit, work):
        def run(i, carry):
            work(i)
            return carry

        lax.fori_loop(0, limit, run, 0)

    ahead = min(4, parts)
    for c in range(ahead):
        load(0, c).start()

    barrier = pltpu.get_barrier_semaphore()
    for axis in count:
        for target in (after[axis], before[axis]):
            pl.semaphore_signal(barrier, inc=1, device_id={axis: target}, device_id_type=MESH)
    pl.semaphore_wait(barrier, 6)

    def first_faces(c):
        load(0, c).wait()

        @pl.when(c < parts - ahead)
        def _():
            load(0, c + ahead).start()

        send_faces(0, c)
        load(1, c).start()
        load(2, c).start()

    each(parts, first_faces)

    level = lax.broadcasted_iota(jnp.int32, (wide, deep, members), 1)

    def tall(values):
        return jnp.broadcast_to(values[:, None, :], (wide, deep, members))

    def advanced(p, y, c):
        middle = field[p, y + 1, inner(c)]
        first = tall(zhalo[p, 0, y, span(c)])
        last = tall(zhalo[p, 1, y, span(c)])
        lower = jnp.where(level == 0, first, pltpu.roll(middle, 1, 1))
        upper = jnp.where(level == deep - 1, last, pltpu.roll(middle, deep - 1, 1))
        spread = (
            field[p, y, inner(c)] + field[p, y + 2, inner(c)]
            + field[p, y + 1, inner(c, -1)] + field[p, y + 1, inner(c, 1)]
            + (lower + upper) - 6.0 * middle
        )
        return middle + coeff[y, span(c)] * spread + gain[y, span(c)]

    def step(t, carry):
        old, new = lax.rem(t, 2), lax.rem(t + 1, 2)

        def chunk(c):
            @pl.when(t == 0)
            def _():
                load(1, c).wait()
                load(2, c).wait()

            @pl.when(t > 0)
            def _():
                wait_sent(t - 1, c)

            wait_faces(t, c)

            def row(y):
                field[new, y + 1, inner(c)] = advanced(old, y, c)

            each(rows_y, row)
            send_faces(t + 1, c)

        each(parts, chunk)
        return carry

    lax.fori_loop(0, LAST, step, 0)

    def last_chunk(c):
        wait_faces(LAST, c)

        def row(y):
            block = advanced(LAST % 2, y, c)
            end[y, span(c)] = block
            reach = 1
            while reach < deep:
                block = block + jnp.where(level >= reach, pltpu.roll(block, reach, 1), 0.0)
                reach *= 2
            running[y, span(c)] = block * scale

        each(rows_y, row)

        @pl.when(mine["pz"] > 0)
        def _():
            prefix_copy(c).wait_recv()

            def lift(y):
                running[y, span(c)] = running[y, span(c)] + tall(entering[y, span(c)])

            each(rows_y, lift)

        @pl.when(jnp.logical_not(highest))
        def _():
            prefix_copy(c).start()

        @pl.when(jnp.logical_and(lowest, c >= behind))
        def _():
            z_copy(LAST, 1, c - behind).start()

    each(parts, last_chunk)

    @pl.when(lowest)
    def _():
        each(behind, lambda c: z_copy(LAST, 1, parts - behind + c).start())

    def finish(c):
        wait_sent(LAST - 1, c)
        wait_sent(LAST, c)

        @pl.when(jnp.logical_not(highest))
        def _():
            prefix_copy(c).wait_send()

    each(parts, finish)


def store(end, running, tracer_end, potential, sem):
    rows_y = end.shape[0]
    pieces = next(n for n in (4, 2, 1) if rows_y % n == 0)
    copies = []
    for i in range(pieces):
        part = pl.ds(i * (rows_y // pieces), rows_y // pieces)
        copies.append(pltpu.make_async_copy(end.at[part], tracer_end.at[part], sem.at[0, i]))
        copies.append(pltpu.make_async_copy(running.at[part], potential.at[part], sem.at[1, i]))
    for copy in copies:
        copy.start()
    for copy in copies:
        copy.wait()


def on_device(counts, tracer, conductance, source):
    shape = tracer.shape
    rows_y, cells, deep, members = shape
    parts = chunks_of(cells)
    anywhere = pl.BlockSpec(memory_space=pl.ANY)
    near = pl.BlockSpec(memory_space=pltpu.VMEM)
    f32 = jnp.float32
    dma = pltpu.SemaphoreType.DMA
    end, running = pl.pallas_call(
        functools.partial(evolve, counts, parts),
        out_shape=(pltpu.VMEM(shape, f32), pltpu.VMEM(shape, f32)),
        in_specs=[anywhere] * 3,
        out_specs=(near, near),
        scratch_shapes=[
            pltpu.VMEM((2, rows_y + 2, cells + 2, deep, members), f32),
            pltpu.VMEM(shape, f32),
            pltpu.VMEM(shape, f32),
            pltpu.VMEM((2, 2, rows_y, cells, members), f32),
            pltpu.VMEM((rows_y, cells, members), f32),
            dma((3, parts)),
            dma((2, 2, parts)), dma((2, 2, parts)),
            dma((2, 2, parts)), dma((2, 2, parts)),
            dma((2, 2)), dma((2, 2)),
            dma((parts,)), dma((parts,)),
        ],
        compiler_params=pltpu.CompilerParams(
            collective_id=0, has_side_effects=True, vmem_limit_bytes=44 * 1024 * 1024
        ),
        name="evolve",
    )(tracer, conductance, source)
    tracer_end, potential = pl.pallas_call(
        store,
        out_shape=(jax.ShapeDtypeStruct(shape, f32),) * 2,
        in_specs=[near, near],
        out_specs=(anywhere, anywhere),
        scratch_shapes=[dma((2, 4))],
        compiler_params=pltpu.CompilerParams(vmem_limit_bytes=1024 * 1024),
        name="store",
    )(end, running)
    return potential, tracer_end


def solution(mesh):
    placed = P(*AXES, None)
    counts = tuple(mesh.shape[axis] for axis in AXES)
    return jax.shard_map(
        functools.partial(on_device, counts),
        mesh=mesh,
        in_specs=(placed,) * 3,
        out_specs=(placed,) * 2,
        check_vma=False,
    )
```

```python
import functools

import jax
import jax.numpy as jnp
from jax import lax
from jax.experimental import pallas as pl
from jax.experimental.pallas import tpu as pltpu
from jax.sharding import PartitionSpec as P

STEPS = 4
LAST = STEPS - 1
AXES = ("py", "px", "pz")
MESH = pl.DeviceIdType.MESH


def chunks_of(cells):
    for parts in (16, 8, 4, 2):
        if cells % (8 * parts) == 0:
            return parts
    raise ValueError("x extent")


def evolve(
    counts, parts, bands, tracer, conductance, source, end, running,
    field, coeff, gain, zhalo, entering,
    load_sem, zsend, zrecv, ysend, yrecv, xsend, xrecv, psend, precv,
):
    rows_y, cells, deep, members = tracer.shape
    wide = cells // parts
    broad = cells // bands
    per_band = parts // bands
    ahead = load_sem.shape[0] - 2
    pieces = precv.shape[0] - parts + 1
    thick = rows_y // pieces
    early = parts * 3 // 8
    scale = 1.0 / (deep * counts[2])
    count = dict(zip(AXES, counts))
    mine = {axis: lax.axis_index(axis) for axis in count}
    after = {axis: lax.rem(mine[axis] + 1, count[axis]) for axis in count}
    before = {axis: lax.rem(mine[axis] + count[axis] - 1, count[axis]) for axis in count}
    lowest = mine["pz"] == 0
    highest = mine["pz"] == count["pz"] - 1
    held = jnp.clip(count["pz"] - 2 - mine["pz"], 0, 2) * (parts // 4)
    body_y = pl.ds(1, rows_y)
    body_x = pl.ds(1, cells)

    def span(c):
        return pl.ds(pl.multiple_of(c * wide, 8), wide)

    def inner(c, shift=0):
        return pl.ds(c * wide + 1 + shift, wide)

    def load(c):
        return pltpu.make_async_copy(
            tracer.at[:, span(c)], field.at[0, body_y, inner(c)], load_sem.at[lax.rem(c, ahead)]
        )

    def load_rest():
        return (
            pltpu.make_async_copy(conductance, coeff, load_sem.at[ahead]),
            pltpu.make_async_copy(source, gain, load_sem.at[ahead + 1]),
        )

    def remote(src, dst, send, recv, axis, target):
        return pltpu.make_async_remote_copy(
            src_ref=src, dst_ref=dst, send_sem=send, recv_sem=recv,
            device_id={axis: target}, device_id_type=MESH,
        )

    def z_copy(t, side, c):
        p = lax.rem(t, 2)
        return remote(
            field.at[p, body_y, inner(c), (deep - 1, 0)[side]],
            zhalo.at[p, side, :, span(c)],
            zsend.at[p, side], zrecv.at[p, c],
            "pz", (after, before)[side]["pz"],
        )

    def z_both(t, c):
        p = lax.rem(t, 2)
        both = zhalo.at[p, :, :, span(c)]
        return remote(both, both, zsend.at[p, 0], zrecv.at[p, c], "pz", after["pz"])

    def z_whole(t, side):
        p = lax.rem(t, 2)
        return remote(
            field.at[p, body_y, body_x, (deep - 1, 0)[side]],
            zhalo.at[p, side],
            zsend.at[p, side], zrecv.at[p, 0],
            "pz", (after, before)[side]["pz"],
        )

    def y_copy(t, side, b, where=None):
        p = lax.rem(t, 2)
        where = pl.ds(b * broad + 1, broad) if where is None else where
        return remote(
            field.at[p, (rows_y, 1)[side], where],
            field.at[p, (0, rows_y + 1)[side], where],
            ysend.at[p, side], yrecv.at[p, side, b],
            "py", (after, before)[side]["py"],
        )

    def x_copy(t, side):
        p = lax.rem(t, 2)
        return remote(
            field.at[p, body_y, (cells, 1)[side]],
            field.at[p, body_y, (0, cells + 1)[side]],
            xsend.at[p, side], xrecv.at[p, side],
            "px", (after, before)[side]["px"],
        )

    def prefix_copy(c, first, number, recv):
        part = pl.ds(first, number)
        return remote(
            running.at[part, span(c), deep - 1], entering.at[part, span(c)],
            psend, precv.at[recv], "pz", after["pz"],
        )

    def prefix_whole():
        return remote(
            running.at[:, :, deep - 1], entering, psend, precv.at[0], "pz", after["pz"]
        )

    def send_faces(t, c):
        @pl.when((t < LAST) | (c < parts - held))
        def _():
            z_copy(t, 0, c).start()

        @pl.when((t < LAST) | (mine["pz"] > 0) | (c < early))
        def _():
            z_copy(t, 1, c).start()

        @pl.when(lax.rem(c, per_band) == per_band - 1)
        def _():
            for side in (0, 1):
                y_copy(t, side, lax.div(c, per_band)).start()

        @pl.when(c == 0)
        def _():
            x_copy(t, 1).start()

        @pl.when(c == parts - 1)
        def _():
            x_copy(t, 0).start()

    def wait_sent(t):
        for side in (0, 1):
            z_whole(t, side).wait_send()
            y_copy(t, side, 0, body_x).wait_send()
            x_copy(t, side).wait_send()

    def wait_faces(t, c):
        z_both(t, c).wait_recv()

        @pl.when(lax.rem(c, per_band) == 0)
        def _():
            for side in (0, 1):
                y_copy(t, side, lax.div(c, per_band)).wait_recv()

        @pl.when(c == 0)
        def _():
            x_copy(t, 0).wait_recv()

        @pl.when(c == parts - 1)
        def _():
            x_copy(t, 1).wait_recv()

    def each(limit, work):
        def run(i, carry):
            work(i)
            return carry

        lax.fori_loop(0, limit, run, 0)

    for c in range(ahead):
        load(c).start()

    barrier = pltpu.get_barrier_semaphore()
    for axis in count:
        for target in (after[axis], before[axis]):
            pl.semaphore_signal(barrier, inc=1, device_id={axis: target}, device_id_type=MESH)
    pl.semaphore_wait(barrier, 6)

    def first_faces(c):
        load(c).wait()

        @pl.when(c < parts - ahead)
        def _():
            load(c + ahead).start()

        @pl.when(c == parts - ahead)
        def _():
            for copy in load_rest():
                copy.start()

        send_faces(0, c)

    each(parts, first_faces)
    for copy in load_rest():
        copy.wait()

    level = lax.broadcasted_iota(jnp.int32, (wide, deep, members), 1)

    def tall(values):
        return jnp.broadcast_to(values[:, None, :], (wide, deep, members))

    def advanced(p, y, c):
        middle = field[p, y + 1, inner(c)]
        first = tall(zhalo[p, 0, y, span(c)])
        last = tall(zhalo[p, 1, y, span(c)])
        lower = jnp.where(level == 0, first, pltpu.roll(middle, 1, 1))
        upper = jnp.where(level == deep - 1, last, pltpu.roll(middle, deep - 1, 1))
        spread = (
            field[p, y, inner(c)] + field[p, y + 2, inner(c)]
            + field[p, y + 1, inner(c, -1)] + field[p, y + 1, inner(c, 1)]
            + (lower + upper) - 6.0 * middle
        )
        return middle + coeff[y, span(c)] * spread + gain[y, span(c)]

    def step(t, carry):
        old, new = lax.rem(t, 2), lax.rem(t + 1, 2)

        @pl.when(t > 0)
        def _():
            wait_sent(t - 1)

        def chunk(c):
            wait_faces(t, c)

            def row(y):
                field[new, y + 1, inner(c)] = advanced(old, y, c)

            each(rows_y, row)
            send_faces(t + 1, c)

        each(parts, chunk)
        return carry

    lax.fori_loop(0, LAST, step, 0)

    def finish_chunk(c):
        wait_faces(LAST, c)

        def row(y):
            block = advanced(LAST % 2, y, c)
            end[y, span(c)] = block
            reach = 1
            while reach < deep:
                block = block + jnp.where(level >= reach, pltpu.roll(block, reach, 1), 0.0)
                reach *= 2
            running[y, span(c)] = block * scale

        each(rows_y, row)

    def pass_on(c, first, number, recv):
        copy = prefix_copy(c, first, number, recv)

        @pl.when(jnp.logical_not(lowest))
        def _():
            copy.wait_recv()

            def lift(i):
                y = first + i
                running[y, span(c)] = running[y, span(c)] + tall(entering[y, span(c)])

            each(number, lift)

        @pl.when(jnp.logical_not(highest))
        def _():
            copy.start()

    def late_faces(c):
        @pl.when(c < held)
        def _():
            z_copy(LAST, 0, parts - held + c).start()

        @pl.when(lowest & (c >= early))
        def _():
            z_copy(LAST, 1, c).start()

    finish_chunk(0)

    def last_chunk(i):
        finish_chunk(i + 1)
        pass_on(i, 0, rows_y, i)
        late_faces(i)

    each(parts - 1, last_chunk)
    each(pieces, lambda h: pass_on(parts - 1, h * thick, thick, parts - 1 + h))
    late_faces(parts - 1)

    wait_sent(LAST - 1)
    wait_sent(LAST)

    @pl.when(jnp.logical_not(highest))
    def _():
        prefix_whole().wait_send()


def store(end, running, tracer_end, potential, sem):
    rows_y = end.shape[0]
    pieces = next(n for n in (4, 2, 1) if rows_y % n == 0)
    copies = []
    for i in range(pieces):
        part = pl.ds(i * (rows_y // pieces), rows_y // pieces)
        copies.append(pltpu.make_async_copy(end.at[part], tracer_end.at[part], sem.at[0, i]))
        copies.append(pltpu.make_async_copy(running.at[part], potential.at[part], sem.at[1, i]))
    for copy in copies:
        copy.start()
    for copy in copies:
        copy.wait()


def on_device(counts, tracer, conductance, source):
    shape = tracer.shape
    rows_y, cells, deep, members = shape
    parts = chunks_of(cells)
    bands = min(4, parts)
    pieces = next(n for n in (4, 2, 1) if rows_y % n == 0)
    anywhere = pl.BlockSpec(memory_space=pl.ANY)
    near = pl.BlockSpec(memory_space=pltpu.VMEM)
    f32 = jnp.float32
    dma = pltpu.SemaphoreType.DMA
    end, running = pl.pallas_call(
        functools.partial(evolve, counts, parts, bands),
        out_shape=(pltpu.VMEM(shape, f32), pltpu.VMEM(shape, f32)),
        in_specs=[anywhere] * 3,
        out_specs=(near, near),
        scratch_shapes=[
            pltpu.VMEM((2, rows_y + 2, cells + 2, deep, members), f32),
            pltpu.VMEM(shape, f32),
            pltpu.VMEM(shape, f32),
            pltpu.VMEM((2, 2, rows_y, cells, members), f32),
            pltpu.VMEM((rows_y, cells, members), f32),
            dma((min(4, parts) + 2,)),
            dma((2, 2)), dma((2, parts)),
            dma((2, 2)), dma((2, 2, bands)),
            dma((2, 2)), dma((2, 2)),
            dma(()), dma((parts - 1 + pieces,)),
        ],
        compiler_params=pltpu.CompilerParams(
            collective_id=0, has_side_effects=True, vmem_limit_bytes=44 * 1024 * 1024
        ),
        name="evolve",
    )(tracer, conductance, source)
    tracer_end, potential = pl.pallas_call(
        store,
        out_shape=(jax.ShapeDtypeStruct(shape, f32),) * 2,
        in_specs=[near, near],
        out_specs=(anywhere, anywhere),
        scratch_shapes=[dma((2, 4))],
        compiler_params=pltpu.CompilerParams(vmem_limit_bytes=1024 * 1024),
        name="store",
    )(end, running)
    return potential, tracer_end


def solution(mesh):
    placed = P(*AXES, None)
    counts = tuple(mesh.shape[axis] for axis in AXES)
    return jax.shard_map(
        functools.partial(on_device, counts),
        mesh=mesh,
        in_specs=(placed,) * 3,
        out_specs=(placed,) * 2,
        check_vma=False,
    )
```

```python
import functools

import jax
import jax.numpy as jnp
from jax import lax
from jax.experimental import pallas as pl
from jax.experimental.pallas import tpu as pltpu
from jax.sharding import PartitionSpec as P

STEPS = 4
LAST = STEPS - 1
EARLY = 6
HOLD = 4
FINE = 3
LEAD = 6
LAG0 = 1
LAG1 = 0
AXES = ("py", "px", "pz")
MESH = pl.DeviceIdType.MESH


def chunks_of(cells):
    for parts in (16, 8, 4, 2):
        if cells % (8 * parts) == 0:
            return parts
    raise ValueError("x extent")


def evolve(
    counts, parts, bands, pieces, tracer, conductance, source, end, running,
    field, coeff, gain, zhalo, entering, leaving,
    load_sem, zsend, zrecv, ysend, yrecv, xsend, xrecv, psend, precv,
):
    rows_y, cells, deep, members = tracer.shape
    wide = cells // parts
    broad = cells // bands
    per_band = parts // bands
    ahead = load_sem.shape[0] - 2
    thick = rows_y // pieces
    coarse = parts - (precv.shape[0] - parts) // (pieces - 1)
    early = parts * EARLY // 16
    lead = parts * LEAD // 16
    lag = jnp.where(lax.rem(lax.axis_index('px'), 2) == 0, LAG0, LAG1)
    scale = 1.0 / (deep * counts[2])
    count = dict(zip(AXES, counts))
    mine = {axis: lax.axis_index(axis) for axis in count}
    after = {axis: lax.rem(mine[axis] + 1, count[axis]) for axis in count}
    before = {axis: lax.rem(mine[axis] + count[axis] - 1, count[axis]) for axis in count}
    lowest = mine["pz"] == 0
    highest = mine["pz"] == count["pz"] - 1
    held = jnp.clip(count["pz"] - 2 - mine["pz"], 0, 2) * (parts * HOLD // 16)
    body_y = pl.ds(1, rows_y)
    body_x = pl.ds(1, cells)

    def span(c):
        return pl.ds(pl.multiple_of(c * wide, 8), wide)

    def inner(c, shift=0):
        return pl.ds(c * wide + 1 + shift, wide)

    def load(c):
        return pltpu.make_async_copy(
            tracer.at[:, span(c)], field.at[0, body_y, inner(c)], load_sem.at[lax.rem(c, ahead)]
        )

    def load_rest():
        return (
            pltpu.make_async_copy(conductance, coeff, load_sem.at[ahead]),
            pltpu.make_async_copy(source, gain, load_sem.at[ahead + 1]),
        )

    def remote(src, dst, send, recv, axis, target):
        return pltpu.make_async_remote_copy(
            src_ref=src, dst_ref=dst, send_sem=send, recv_sem=recv,
            device_id={axis: target}, device_id_type=MESH,
        )

    def z_copy(t, side, c):
        p = lax.rem(t, 2)
        return remote(
            field.at[p, body_y, inner(c), (deep - 1, 0)[side]],
            zhalo.at[p, side, :, span(c)],
            zsend.at[p, side], zrecv.at[p, c],
            "pz", (after, before)[side]["pz"],
        )

    def z_both(t, c):
        p = lax.rem(t, 2)
        both = zhalo.at[p, :, :, span(c)]
        return remote(both, both, zsend.at[p, 0], zrecv.at[p, c], "pz", after["pz"])

    def z_whole(t, side):
        p = lax.rem(t, 2)
        return remote(
            field.at[p, body_y, body_x, (deep - 1, 0)[side]],
            zhalo.at[p, side],
            zsend.at[p, side], zrecv.at[p, 0],
            "pz", (after, before)[side]["pz"],
        )

    def y_copy(t, side, b, where=None):
        p = lax.rem(t, 2)
        where = pl.ds(b * broad + 1, broad) if where is None else where
        return remote(
            field.at[p, (rows_y, 1)[side], where],
            field.at[p, (0, rows_y + 1)[side], where],
            ysend.at[p, side], yrecv.at[p, side, b],
            "py", (after, before)[side]["py"],
        )

    def x_copy(t, side):
        p = lax.rem(t, 2)
        return remote(
            field.at[p, body_y, (cells, 1)[side]],
            field.at[p, body_y, (0, cells + 1)[side]],
            xsend.at[p, side], xrecv.at[p, side],
            "px", (after, before)[side]["px"],
        )

    def prefix_copy(c, first, number, recv):
        part = pl.ds(first, number)
        return remote(
            leaving.at[part, span(c)], entering.at[part, span(c)],
            psend, precv.at[recv], "pz", after["pz"],
        )

    def prefix_whole():
        return remote(leaving, entering, psend, precv.at[0], "pz", after["pz"])

    def send_faces(t, c, wrap=True):
        @pl.when((t < LAST) | (c < parts - held))
        def _():
            z_copy(t, 0, c).start()

        @pl.when(((t < LAST) & wrap) | (mine["pz"] > 0) | ((t == LAST) & (c < early)))
        def _():
            z_copy(t, 1, c).start()

        @pl.when(lax.rem(c, per_band) == per_band - 1)
        def _():
            for side in (0, 1):
                y_copy(t, side, lax.div(c, per_band)).start()

        @pl.when(c == 0)
        def _():
            x_copy(t, 1).start()

        @pl.when(c == parts - 1)
        def _():
            x_copy(t, 0).start()

    def wait_sent(t):
        for side in (0, 1):
            z_whole(t, side).wait_send()
            y_copy(t, side, 0, body_x).wait_send()
            x_copy(t, side).wait_send()

    def wait_faces(t, c):
        z_both(t, c).wait_recv()

        @pl.when(lax.rem(c, per_band) == 0)
        def _():
            for side in (0, 1):
                y_copy(t, side, lax.div(c, per_band)).wait_recv()

        @pl.when(c == 0)
        def _():
            x_copy(t, 0).wait_recv()

        @pl.when(c == parts - 1)
        def _():
            x_copy(t, 1).wait_recv()

    def each(limit, work):
        def run(i, carry):
            work(i)
            return carry

        lax.fori_loop(0, limit, run, 0)

    for c in range(ahead):
        load(c).start()

    barrier = pltpu.get_barrier_semaphore()

    def greet(axis, target):
        pl.semaphore_signal(barrier, inc=1, device_id={axis: target}, device_id_type=MESH)

    for axis in ("pz", "px", "py"):
        pl.when((axis != "pz") | jnp.logical_not(highest))(lambda: greet(axis, after[axis]))
        pl.when((axis != "pz") | jnp.logical_not(lowest))(lambda: greet(axis, before[axis]))

    @pl.when(lowest)
    def _():
        pl.semaphore_wait(barrier, 5)
        greet("pz", before["pz"])

    @pl.when(jnp.logical_not(lowest))
    def _():
        pl.semaphore_wait(barrier, 6)

    @pl.when(highest)
    def _():
        greet("pz", after["pz"])

    def first_faces(c):
        load(c).wait()

        @pl.when(c < parts - ahead)
        def _():
            load(c + ahead).start()

        @pl.when(c == parts - ahead)
        def _():
            for copy in load_rest():
                copy.start()

        send_faces(0, c, c >= lead)

        @pl.when(lowest & (c == lead - 1))
        def _():
            pl.semaphore_wait(barrier, 1)
            each(lead, lambda k: z_copy(0, 1, k).start())

    each(parts, first_faces)
    for copy in load_rest():
        copy.wait()

    level = lax.broadcasted_iota(jnp.int32, (wide, deep, members), 1)

    def tall(values):
        return jnp.broadcast_to(values[:, None, :], (wide, deep, members))

    def advanced(p, y, c):
        middle = field[p, y + 1, inner(c)]
        first = tall(zhalo[p, 0, y, span(c)])
        last = tall(zhalo[p, 1, y, span(c)])
        lower = jnp.where(level == 0, first, pltpu.roll(middle, 1, 1))
        upper = jnp.where(level == deep - 1, last, pltpu.roll(middle, deep - 1, 1))
        spread = (
            field[p, y, inner(c)] + field[p, y + 2, inner(c)]
            + field[p, y + 1, inner(c, -1)] + field[p, y + 1, inner(c, 1)]
            + (lower + upper) - 6.0 * middle
        )
        return middle + coeff[y, span(c)] * spread + gain[y, span(c)]

    def step(t, carry):
        old, new = lax.rem(t, 2), lax.rem(t + 1, 2)

        @pl.when(t > 0)
        def _():
            wait_sent(t - 1)

        def chunk(c):
            wait_faces(t, c)

            def row(y):
                field[new, y + 1, inner(c)] = advanced(old, y, c)

            each(rows_y, row)
            send_faces(t + 1, c)

        each(parts, chunk)
        return carry

    lax.fori_loop(0, LAST, step, 0)

    def finish_chunk(c):
        wait_faces(LAST, c)

        def row(y):
            block = advanced(LAST % 2, y, c)
            end[y, span(c)] = block
            reach = 1
            while reach < deep:
                block = block + jnp.where(level >= reach, pltpu.roll(block, reach, 1), 0.0)
                reach *= 2
            block = block * scale
            running[y, span(c)] = block
            leaving[y, span(c)] = block[:, deep - 1, :]

        each(rows_y, row)

    def pass_on(c, first, number, recv):
        copy = prefix_copy(c, first, number, recv)

        def rows(work):
            each(number, lambda i: work(first + i))

        @pl.when(jnp.logical_not(lowest))
        def _():
            copy.wait_recv()

        @pl.when(jnp.logical_not(lowest | highest))
        def _():
            def add(y):
                leaving[y, span(c)] = leaving[y, span(c)] + entering[y, span(c)]

            rows(add)

        @pl.when(jnp.logical_not(highest))
        def _():
            copy.start()

        @pl.when(jnp.logical_not(lowest))
        def _():
            def lift(y):
                running[y, span(c)] = running[y, span(c)] + tall(entering[y, span(c)])

            rows(lift)

    def wrap_part(c, first, number):
        p = LAST % 2

        @pl.when(lowest & (c >= early))
        def _():
            remote(
                field.at[p, pl.ds(first + 1, number), inner(c), 0],
                zhalo.at[p, 1, pl.ds(first, number), span(c)],
                zsend.at[p, 1], zrecv.at[p, c], "pz", before["pz"],
            ).start()

    finish_chunk(0)

    def coarse_chunk(c):
        finish_chunk(c + 1)
        pass_on(c, 0, rows_y, c)

        @pl.when(c < held)
        def _():
            z_copy(LAST, 0, parts - held + c).start()

        wrap_part(c - lag, 0, rows_y)

    each(coarse, coarse_chunk)

    def fine_chunk(j):
        c = coarse + j
        more = c < parts - 1

        @pl.when(more & jnp.logical_not(highest))
        def _():
            finish_chunk(c + 1)

        def piece(h):
            pass_on(c, h * thick, thick, coarse + j * pieces + h)
            wrap_part(c - lag, h * thick, thick)

        each(pieces, piece)

        @pl.when(more & highest)
        def _():
            finish_chunk(c + 1)

    each(parts - coarse, fine_chunk)
    each(lag, lambda i: wrap_part(parts - lag + i, 0, rows_y))

    wait_sent(LAST - 1)
    wait_sent(LAST)

    @pl.when(jnp.logical_not(highest))
    def _():
        prefix_whole().wait_send()


def store(end, running, tracer_end, potential, sem):
    whole = (
        pltpu.make_async_copy(end, tracer_end, sem.at[0]),
        pltpu.make_async_copy(running, potential, sem.at[1]),
    )
    for y in range(end.shape[0]):
        pltpu.make_async_copy(end.at[y], tracer_end.at[y], sem.at[0]).start()
        pltpu.make_async_copy(running.at[y], potential.at[y], sem.at[1]).start()
    for copy in whole:
        copy.wait()


def on_device(counts, tracer, conductance, source):
    shape = tracer.shape
    rows_y, cells, deep, members = shape
    parts = chunks_of(cells)
    bands = min(4, parts)
    pieces = next(n for n in (4, 2, 1) if rows_y % n == 0)
    anywhere = pl.BlockSpec(memory_space=pl.ANY)
    near = pl.BlockSpec(memory_space=pltpu.VMEM)
    f32 = jnp.float32
    dma = pltpu.SemaphoreType.DMA
    end, running = pl.pallas_call(
        functools.partial(evolve, counts, parts, bands, pieces),
        out_shape=(pltpu.VMEM(shape, f32), pltpu.VMEM(shape, f32)),
        in_specs=[anywhere] * 3,
        out_specs=(near, near),
        scratch_shapes=[
            pltpu.VMEM((2, rows_y + 2, cells + 2, deep, members), f32),
            pltpu.VMEM(shape, f32),
            pltpu.VMEM(shape, f32),
            pltpu.VMEM((2, 2, rows_y, cells, members), f32),
            pltpu.VMEM((rows_y, cells, members), f32),
            pltpu.VMEM((rows_y, cells, members), f32),
            dma((min(4, parts) + 2,)),
            dma((2, 2)), dma((2, parts)),
            dma((2, 2)), dma((2, 2, bands)),
            dma((2, 2)), dma((2, 2)),
            dma(()), dma((parts + FINE * (pieces - 1),)),
        ],
        compiler_params=pltpu.CompilerParams(
            collective_id=0, has_side_effects=True, vmem_limit_bytes=46 * 1024 * 1024
        ),
        name="evolve",
    )(tracer, conductance, source)
    tracer_end, potential = pl.pallas_call(
        store,
        out_shape=(jax.ShapeDtypeStruct(shape, f32),) * 2,
        in_specs=[near, near],
        out_specs=(anywhere, anywhere),
        scratch_shapes=[dma((2,))],
        compiler_params=pltpu.CompilerParams(vmem_limit_bytes=1024 * 1024),
        name="store",
    )(end, running)
    return potential, tracer_end


def solution(mesh):
    placed = P(*AXES, None)
    counts = tuple(mesh.shape[axis] for axis in AXES)
    return jax.shard_map(
        functools.partial(on_device, counts),
        mesh=mesh,
        in_specs=(placed,) * 3,
        out_specs=(placed,) * 2,
        check_vma=False,
    )
```

```python
import functools

import jax
import jax.numpy as jnp
from jax import lax
from jax.experimental import pallas as pl
from jax.experimental.pallas import tpu as pltpu
from jax.sharding import PartitionSpec as P

STEPS = 4
LAST = STEPS - 1
EARLY = 6
HOLD = 4
FINE = 3
PIECES = 4
BANDS = 2
LEAD = 6
LAG0 = 1
LAG1 = 0
AXES = ("py", "px", "pz")
MESH = pl.DeviceIdType.MESH


def chunks_of(cells):
    for parts in (16, 8, 4, 2):
        if cells % (8 * parts) == 0:
            return parts
    raise ValueError("x extent")


def evolve(
    counts, parts, bands, pieces, tracer, conductance, source, end, running,
    field, coeff, gain, zhalo, entering, leaving,
    load_sem, zsend, zrecv, ysend, yrecv, xsend, xrecv, psend, precv,
):
    rows_y, cells, deep, members = tracer.shape
    wide = cells // parts
    broad = cells // bands
    per_band = parts // bands
    ahead = load_sem.shape[0] - 2
    thick = rows_y // pieces
    coarse = parts - (precv.shape[0] - parts) // (pieces - 1)
    early = parts * EARLY // 16
    lead = parts * LEAD // 16
    lag = jnp.where(lax.rem(lax.axis_index('px'), 2) == 0, LAG0, LAG1)
    scale = 1.0 / (deep * counts[2])
    count = dict(zip(AXES, counts))
    mine = {axis: lax.axis_index(axis) for axis in count}
    after = {axis: lax.rem(mine[axis] + 1, count[axis]) for axis in count}
    before = {axis: lax.rem(mine[axis] + count[axis] - 1, count[axis]) for axis in count}
    lowest = mine["pz"] == 0
    highest = mine["pz"] == count["pz"] - 1
    held = jnp.clip(count["pz"] - 2 - mine["pz"], 0, 2) * (parts * HOLD // 16)
    body_y = pl.ds(1, rows_y)
    body_x = pl.ds(1, cells)

    def span(c):
        return pl.ds(pl.multiple_of(c * wide, 8), wide)

    def inner(c, shift=0):
        return pl.ds(c * wide + 1 + shift, wide)

    def load(c):
        return pltpu.make_async_copy(
            tracer.at[:, span(c)], field.at[0, body_y, inner(c)], load_sem.at[lax.rem(c, ahead)]
        )

    def load_rest():
        return (
            pltpu.make_async_copy(conductance, coeff, load_sem.at[ahead]),
            pltpu.make_async_copy(source, gain, load_sem.at[ahead + 1]),
        )

    def remote(src, dst, send, recv, axis, target):
        return pltpu.make_async_remote_copy(
            src_ref=src, dst_ref=dst, send_sem=send, recv_sem=recv,
            device_id={axis: target}, device_id_type=MESH,
        )

    paired = max(parts - 4, 0)

    def z_slot(c):
        return jnp.where(c < paired, lax.div(c, 2), c - paired // 2)

    def z_copy(t, side, c):
        p = lax.rem(t, 2)
        return remote(
            field.at[p, body_y, inner(c), (deep - 1, 0)[side]],
            zhalo.at[p, side, :, span(c)],
            zsend.at[p, side], zrecv.at[p, z_slot(c)],
            "pz", (after, before)[side]["pz"],
        )

    def z_both(t, c, chunks):
        p = lax.rem(t, 2)
        both = zhalo.at[p, :, :, pl.ds(pl.multiple_of(c * wide, 8), chunks * wide)]
        return remote(both, both, zsend.at[p, 0], zrecv.at[p, z_slot(c)], "pz", after["pz"])

    def z_whole(t, side):
        p = lax.rem(t, 2)
        return remote(
            field.at[p, body_y, body_x, (deep - 1, 0)[side]],
            zhalo.at[p, side],
            zsend.at[p, side], zrecv.at[p, 0],
            "pz", (after, before)[side]["pz"],
        )

    def y_copy(t, side, b, where=None):
        p = lax.rem(t, 2)
        where = pl.ds(b * broad + 1, broad) if where is None else where
        return remote(
            field.at[p, (rows_y, 1)[side], where],
            field.at[p, (0, rows_y + 1)[side], where],
            ysend.at[p, side], yrecv.at[p, side, b],
            "py", (after, before)[side]["py"],
        )

    def x_copy(t, side):
        p = lax.rem(t, 2)
        return remote(
            field.at[p, body_y, (cells, 1)[side]],
            field.at[p, body_y, (0, cells + 1)[side]],
            xsend.at[p, side], xrecv.at[p, side],
            "px", (after, before)[side]["px"],
        )

    def prefix_copy(c, first, number, recv):
        part = pl.ds(first, number)
        return remote(
            leaving.at[part, span(c)], entering.at[part, span(c)],
            psend, precv.at[recv], "pz", after["pz"],
        )

    def prefix_whole():
        return remote(leaving, entering, psend, precv.at[0], "pz", after["pz"])

    def send_faces(t, c, wrap=True):
        @pl.when((t < LAST) | (c < parts - held))
        def _():
            z_copy(t, 0, c).start()

        @pl.when(((t < LAST) & wrap) | (mine["pz"] > 0) | ((t == LAST) & (c < early)))
        def _():
            z_copy(t, 1, c).start()

        @pl.when(lax.rem(c, per_band) == per_band - 1)
        def _():
            for side in (0, 1):
                y_copy(t, side, lax.div(c, per_band)).start()

        @pl.when(c == 0)
        def _():
            x_copy(t, 1).start()

        @pl.when(c == parts - 1)
        def _():
            x_copy(t, 0).start()

    def wait_sent(t):
        for side in (0, 1):
            z_whole(t, side).wait_send()
            y_copy(t, side, 0, body_x).wait_send()
            x_copy(t, side).wait_send()

    def wait_faces(t, c):
        @pl.when(c >= paired)
        def _():
            z_both(t, c, 1).wait_recv()

        if paired:
            @pl.when((c < paired) & (lax.rem(c, 2) == 0))
            def _():
                z_both(t, c, 2).wait_recv()

        @pl.when(lax.rem(c, per_band) == 0)
        def _():
            for side in (0, 1):
                y_copy(t, side, lax.div(c, per_band)).wait_recv()

        @pl.when(c == 0)
        def _():
            x_copy(t, 0).wait_recv()

        @pl.when(c == parts - 1)
        def _():
            x_copy(t, 1).wait_recv()

    def each(limit, work):
        def run(i, carry):
            work(i)
            return carry

        lax.fori_loop(0, limit, run, 0)

    for c in range(ahead):
        load(c).start()

    barrier = pltpu.get_barrier_semaphore()

    def greet(axis, target):
        pl.semaphore_signal(barrier, inc=1, device_id={axis: target}, device_id_type=MESH)

    for axis in ("pz", "px", "py"):
        pl.when((axis != "pz") | jnp.logical_not(highest))(lambda: greet(axis, after[axis]))
        pl.when((axis != "pz") | jnp.logical_not(lowest))(lambda: greet(axis, before[axis]))

    @pl.when(lowest)
    def _():
        pl.semaphore_wait(barrier, 5)
        greet("pz", before["pz"])

    @pl.when(jnp.logical_not(lowest))
    def _():
        pl.semaphore_wait(barrier, 6)

    @pl.when(highest)
    def _():
        greet("pz", after["pz"])

    def first_faces(c):
        load(c).wait()

        @pl.when(c < parts - ahead)
        def _():
            load(c + ahead).start()

        @pl.when(c == parts - ahead)
        def _():
            for copy in load_rest():
                copy.start()

        send_faces(0, c, c >= lead)

        @pl.when(lowest & (c == lead - 1))
        def _():
            pl.semaphore_wait(barrier, 1)
            each(lead, lambda k: z_copy(0, 1, k).start())

    each(parts, first_faces)
    for copy in load_rest():
        copy.wait()

    level = lax.broadcasted_iota(jnp.int32, (wide, deep, members), 1)

    def tall(values):
        return jnp.broadcast_to(values[:, None, :], (wide, deep, members))

    def advanced(p, y, c):
        middle = field[p, y + 1, inner(c)]
        first = tall(zhalo[p, 0, y, span(c)])
        last = tall(zhalo[p, 1, y, span(c)])
        lower = jnp.where(level == 0, first, pltpu.roll(middle, 1, 1))
        upper = jnp.where(level == deep - 1, last, pltpu.roll(middle, deep - 1, 1))
        spread = (
            field[p, y, inner(c)] + field[p, y + 2, inner(c)]
            + field[p, y + 1, inner(c, -1)] + field[p, y + 1, inner(c, 1)]
            + (lower + upper) - 6.0 * middle
        )
        return middle + coeff[y, span(c)] * spread + gain[y, span(c)]

    def step(t, carry):
        old, new = lax.rem(t, 2), lax.rem(t + 1, 2)

        @pl.when(t > 0)
        def _():
            wait_sent(t - 1)

        def chunk(c):
            wait_faces(t, c)

            def row(y):
                field[new, y + 1, inner(c)] = advanced(old, y, c)

            each(rows_y, row)
            send_faces(t + 1, c)

        each(parts, chunk)
        return carry

    lax.fori_loop(0, LAST, step, 0)

    def finish_chunk(c):
        wait_faces(LAST, c)

        def row(y):
            block = advanced(LAST % 2, y, c)
            end[y, span(c)] = block
            reach = 1
            while reach < deep:
                block = block + jnp.where(level >= reach, pltpu.roll(block, reach, 1), 0.0)
                reach *= 2
            block = block * scale
            running[y, span(c)] = block
            leaving[y, span(c)] = block[:, deep - 1, :]

        each(rows_y, row)

    def pass_on(c, first, number, recv):
        copy = prefix_copy(c, first, number, recv)

        def rows(work):
            each(number, lambda i: work(first + i))

        @pl.when(jnp.logical_not(lowest))
        def _():
            copy.wait_recv()

        @pl.when(jnp.logical_not(lowest | highest))
        def _():
            def add(y):
                leaving[y, span(c)] = leaving[y, span(c)] + entering[y, span(c)]

            rows(add)

        @pl.when(jnp.logical_not(highest))
        def _():
            copy.start()

        @pl.when(jnp.logical_not(lowest))
        def _():
            def lift(y):
                running[y, span(c)] = running[y, span(c)] + tall(entering[y, span(c)])

            rows(lift)

    def wrap_part(c, first, number):
        p = LAST % 2

        @pl.when(lowest & (c >= early) & (c < parts))
        def _():
            remote(
                field.at[p, pl.ds(first + 1, number), inner(c), 0],
                zhalo.at[p, 1, pl.ds(first, number), span(c)],
                zsend.at[p, 1], zrecv.at[p, z_slot(c)], "pz", before["pz"],
            ).start()

    finish_chunk(0)

    def coarse_chunk(c):
        finish_chunk(c + 1)
        pass_on(c, 0, rows_y, c)

        @pl.when(c < held)
        def _():
            z_copy(LAST, 0, parts - held + c).start()

        wrap_part(c - lag, 0, rows_y)

    each(coarse, coarse_chunk)

    def fine_chunk(j):
        c = coarse + j
        more = c < parts - 1

        @pl.when(more & jnp.logical_not(highest))
        def _():
            finish_chunk(c + 1)

        def piece(h):
            pass_on(c, h * thick, thick, coarse + j * pieces + h)
            wrap_part(c - lag, h * thick, thick)

        each(pieces, piece)

        @pl.when(more & highest)
        def _():
            finish_chunk(c + 1)

    each(parts - coarse, fine_chunk)
    each(lag, lambda i: wrap_part(parts - lag + i, 0, rows_y))

    wait_sent(LAST - 1)
    wait_sent(LAST)

    @pl.when(jnp.logical_not(highest))
    def _():
        prefix_whole().wait_send()


def store(end, running, tracer_end, potential, sem):
    whole = (
        pltpu.make_async_copy(end, tracer_end, sem.at[0]),
        pltpu.make_async_copy(running, potential, sem.at[1]),
    )
    for y in range(end.shape[0]):
        pltpu.make_async_copy(end.at[y], tracer_end.at[y], sem.at[0]).start()
        pltpu.make_async_copy(running.at[y], potential.at[y], sem.at[1]).start()
    for copy in whole:
        copy.wait()


def on_device(counts, tracer, conductance, source):
    shape = tracer.shape
    rows_y, cells, deep, members = shape
    parts = chunks_of(cells)
    bands = min(BANDS, parts)
    pieces = next(n for n in (PIECES, 4, 2, 1) if rows_y % n == 0)
    anywhere = pl.BlockSpec(memory_space=pl.ANY)
    near = pl.BlockSpec(memory_space=pltpu.VMEM)
    f32 = jnp.float32
    dma = pltpu.SemaphoreType.DMA
    end, running = pl.pallas_call(
        functools.partial(evolve, counts, parts, bands, pieces),
        out_shape=(pltpu.VMEM(shape, f32), pltpu.VMEM(shape, f32)),
        in_specs=[anywhere] * 3,
        out_specs=(near, near),
        scratch_shapes=[
            pltpu.VMEM((2, rows_y + 2, cells + 2, deep, members), f32),
            pltpu.VMEM(shape, f32),
            pltpu.VMEM(shape, f32),
            pltpu.VMEM((2, 2, rows_y, cells, members), f32),
            pltpu.VMEM((rows_y, cells, members), f32),
            pltpu.VMEM((rows_y, cells, members), f32),
            dma((min(4, parts) + 2,)),
            dma((2, 2)), dma((2, parts - max(parts - 4, 0) // 2)),
            dma((2, 2)), dma((2, 2, bands)),
            dma((2, 2)), dma((2, 2)),
            dma(()), dma((parts + FINE * (pieces - 1),)),
        ],
        compiler_params=pltpu.CompilerParams(
            collective_id=0, has_side_effects=True, vmem_limit_bytes=46 * 1024 * 1024
        ),
        name="evolve",
    )(tracer, conductance, source)
    tracer_end, potential = pl.pallas_call(
        store,
        out_shape=(jax.ShapeDtypeStruct(shape, f32),) * 2,
        in_specs=[near, near],
        out_specs=(anywhere, anywhere),
        scratch_shapes=[dma((2,))],
        compiler_params=pltpu.CompilerParams(vmem_limit_bytes=1024 * 1024),
        name="store",
    )(end, running)
    return potential, tracer_end


def solution(mesh):
    placed = P(*AXES, None)
    counts = tuple(mesh.shape[axis] for axis in AXES)
    return jax.shard_map(
        functools.partial(on_device, counts),
        mesh=mesh,
        in_specs=(placed,) * 3,
        out_specs=(placed,) * 2,
        check_vma=False,
    )
```
